128 devices in a mesh: cache: 16 (over x, z), expert: 8 (over y, core).
Axes of the slice: x: 4, y: 4, z: 4, core: 2. Of those that a mesh axis runs over, the one named last changes fastest.
Arguments:
- query: bfloat16 [1024, 4096], P('cache', 'expert'), may hold values from -8 to 8
- new_key: bfloat16 [1024, 1024], P('cache', 'expert'), may hold values from -8 to 8
- new_value: bfloat16 [1024, 1024], P('cache', 'expert'), may hold values from -6 to 6
- private_keys: bfloat16 [1024, 64, 1024], P('cache', None, 'expert'), may hold values from -8 to 8
- private_values: bfloat16 [1024, 64, 1024], P('cache', None, 'expert'), may hold values from -6 to 6
- private_lengths: int32 [1024], P('cache'), may hold values from 1 to 64
- prefix_keys: bfloat16 [32, 1024, 1024], P('cache', None, 'expert'), may hold values from -8 to 8
- prefix_values: bfloat16 [32, 1024, 1024], P('cache', None, 'expert'), may hold values from -6 to 6
- slot_group: int32 [32], replicated, may hold values from 0 to 31, each once
- group_ids: int32 [1024, 1], P('cache'), may hold values from 0 to 31; in each aligned block of 64 rows (0 to 63, 64 to 127, ...) at most 8 rows name the same one
- out_weight: bfloat16 [4096, 4096], P('expert', 'cache'), may hold values from -0.09375 to 0.09375
- hidden_in: bfloat16 [1024, 4096], P(('cache', 'expert')), may hold values from -6 to 6
- norm_gain: float32 [4096], replicated, may hold values from 0.1 to 1.9
- expert_ids: int32 [1024, 2], P(('cache', 'expert')), may hold values from 0 to 7, all different within a row; in each aligned block of 8 rows (0 to 7, 8 to 15, ...) at most 4 rows name the same one
- gate_weights: float32 [1024, 2], P(('cache', 'expert')), may hold values from 0.1 to 0.9
- w_gate: bfloat16 [8, 4096, 14336], P('expert', None, 'cache'), may hold values from -0.09375 to 0.09375
- w_up: bfloat16 [8, 4096, 14336], P('expert', None, 'cache'), may hold values from -0.09375 to 0.09375
- w_down: bfloat16 [8, 14336, 4096], P('expert', 'cache'), may hold values from -0.046875 to 0.046875
Outputs:
- attention: bfloat16 [1024, 4096], P('cache', 'expert')
- layer_out: bfloat16 [1024, 4096], P(('cache', 'expert'))
The draws below stay inside these ranges and needn't reach their ends.
Inputs may be any that keep to these rules, and one draw needn't show every extreme that they name: `group_ids`: within each aligned block of 64 requests at most 8 name one group. `slot_group`: each group is held by exactly one slot. `private_lengths`: positions 0 to length - 1 of a request's private cache are live. `expert_ids`: each token names two different experts; among the 8 tokens of one device at most 4 name one expert.
All inputs are finite; a program needn't handle non-finite values.
Results may differ from the reference program's by a relative error of at most 0.0095.
Values may be sent and summed in bfloat16 or wider, within the bound.
No kernel may reach another device: no remote copies, remote signals or barrier semaphores. Data moves between devices by JAX's collectives and lax.ppermute only.
A program may use at most 128 MiB of HBM per device.

```python
import math
import jax
import jax.numpy as jnp
import numpy as np
from jax import lax

D = 4096
FF = 14336
HEAD_DIM = 128
QPK = 4
TOP = 2
R_DEV = 64
PRIV = 64
PLEN = 1024
MOSTG = 8
KV_HEADS = 8
HEADS = 32
QW = 4096
KVW = 1024
EXPERTS = 8
REQS = 1024
TOK_DEV = 8
GROUPS = 32
CAPE = 4
N_CACHE = 16
N_EXPERT = 8


def base(key, shape):
    return jnp.clip(jax.random.normal(key, shape, jnp.float32), -6.0, 6.0)


def draw_query(key, part):
    values = base(jax.random.fold_in(key, 11), (REQS, HEADS * HEAD_DIM))
    return values.astype(jnp.bfloat16)


def draw_new_key(key, part):
    values = base(jax.random.fold_in(key, 12), (REQS, KV_HEADS * HEAD_DIM))
    return values.astype(jnp.bfloat16)


def draw_private_keys(key, part):
    values = base(jax.random.fold_in(key, 13), (REQS, PRIV, KV_HEADS * HEAD_DIM))
    return values.astype(jnp.bfloat16)


def draw_prefix_keys(key, part):
    values = base(jax.random.fold_in(key, 14), (GROUPS, PLEN, KV_HEADS * HEAD_DIM))
    return values.astype(jnp.bfloat16)


def touch_ends(drawn, key, low, largest):
    longest = drawn.shape.index(max(drawn.shape))
    spots = []
    for shift in (0, 1):
        where = [jax.random.randint(jax.random.fold_in(key, axis), (), 0, length) for axis, length in enumerate(drawn.shape)]
        where[longest] = (where[longest] + shift) % drawn.shape[longest]
        spots.append(tuple(where))
    return drawn.at[spots[0]].set(low).at[spots[1]].set(largest)


def level_of(own_key, shape, cuts, least, high):
    def one(position, blocks):
        heights = jax.random.uniform(jax.random.fold_in(jax.random.fold_in(own_key, 6), position), (blocks,), jnp.float32, least / len(cuts), high / len(cuts))
        return jnp.repeat(jnp.exp(heights), shape[position] // blocks).reshape((-1,) + (1,) * (len(shape) - position - 1))

    loudness = one(*cuts[0])
    for cut in cuts[1:]:
        loudness = loudness * one(*cut)
    return loudness


def shared_out(stream_key, own, number, rows, number_of, top, bound, skew):
    sequence = jax.random.permutation(stream_key, number_of)
    packed, usual = shares(number_of, rows * top, bound, skew, True), shares(number_of, rows * top, bound, skew, False)
    places = jnp.arange(number_of)

    def named(sizes, turn):
        used = int((sizes > 0).sum())
        fixed = max(1, used // 4)
        passed = fixed + (places - fixed + turn * (used - fixed)) % max(1, number_of - fixed)
        return jnp.zeros((number_of,), jnp.int32).at[sequence[jnp.where(places < fixed, places, passed)]].set(jnp.asarray(sizes, jnp.int32))

    sizes = jnp.where(number % 4 == 0, named(packed, number // 4), named(usual, number - number // 4 - 1))
    mixed = jax.random.permutation(jax.random.fold_in(own, 3), number_of)
    source_of, receiver = mixed[0:number_of // 2 * 2:2], mixed[1:number_of // 2 * 2:2]
    margin = jnp.minimum(sizes[source_of] - 1, bound - sizes[receiver]) // 2
    margin = jnp.where((source_of == sequence[0]) | (receiver == sequence[0]) | (sizes[receiver] == 0), 0, jnp.maximum(margin, 0))
    passed = jax.random.randint(jax.random.fold_in(own, 4), (number_of // 2,), 0, 1 << 20) % (margin + 1)
    sizes = sizes.at[source_of].add(-passed).at[receiver].add(passed)
    items = jnp.searchsorted(jnp.cumsum(sizes), jnp.arange(rows * top), side="right").astype(jnp.int32)
    table = items.reshape(top, rows).T
    table = table[jax.random.permutation(jax.random.fold_in(own, 1), rows)]
    turn = jax.random.randint(jax.random.fold_in(own, 2), (rows, 1), 0, top)
    return jnp.take_along_axis(table, (jnp.arange(top)[None, :] + turn) % top, axis=1)


def shares(number_of, total, most, lean, full):
    weights = [(1 << 20) // math.isqrt(standing ** lean) + 1 for standing in range(1, number_of + 1)]
    largest = most if full else min(most, max(-(-total // number_of), total * weights[0] // sum(weights)))
    least = 1 if total - largest >= number_of - 1 else 0
    given, rest = [largest] + [least] * (number_of - 1), total - largest - least * (number_of - 1)
    while rest > 0:
        free = [i for i in range(1, number_of) if given[i] < largest] or [i for i in range(1, number_of) if given[i] < most]
        mass, left = sum([weights[i] for i in free]), rest
        for i in free:
            extra = min(most - given[i], max(1, left * weights[i] // mass), rest)
            given[i] = given[i] + extra
            rest = rest - extra
    return np.array(given)


def normal_values(rng, dims, width, most, split=(), kind=jnp.bfloat16):
    drawn = width * jax.random.normal(rng, dims, jnp.float32)
    if split:
        drawn = drawn * level_of(rng, dims, split, -0.22, 0.18)
    return jnp.clip(drawn, -most, most).astype(kind)


def setup_inputs(seed: int = 0) -> dict:
    streams_of = jax.random.split(jax.random.key(seed), 19)
    query = draw_query(jax.random.fold_in(streams_of[18], 71), 0)
    new_key = draw_new_key(jax.random.fold_in(streams_of[18], 71), 0)
    new_value = normal_values(streams_of[2], (REQS, KVW), 1.0, 6.0, ((0, 16), (1, 8)))
    private_keys = draw_private_keys(jax.random.fold_in(streams_of[18], 71), 0)
    private_values = normal_values(streams_of[4], (REQS, PRIV, KVW), 1.0, 6.0, ((0, 16), (2, 8)))
    private_lengths = touch_ends(jax.random.randint(streams_of[5], (REQS,), 1, PRIV + 1), jax.random.fold_in(streams_of[5], 1), 1, PRIV).astype(jnp.int32)
    prefix_keys = draw_prefix_keys(jax.random.fold_in(streams_of[18], 71), 0)
    prefix_values = normal_values(streams_of[7], (GROUPS, PLEN, KVW), 1.0, 6.0, ((0, 16), (2, 8)))
    slot_group = jax.random.permutation(streams_of[8], GROUPS).astype(jnp.int32)
    group_ids_keys = jax.random.split(jax.random.fold_in(streams_of[9], 1), REQS // R_DEV)
    group_ids_turns = jax.random.permutation(jax.random.fold_in(streams_of[9], 3), REQS // R_DEV)
    group_ids = jax.vmap(lambda own, number: shared_out(jax.random.fold_in(streams_of[9], 2), own, number, R_DEV, GROUPS, 1, MOSTG, 2))(group_ids_keys, group_ids_turns).reshape((REQS, 1))
    out_weight = normal_values(streams_of[10], (QW, D), QW ** -0.5, 0.09375, ((0, 8), (1, 16)))
    hidden_in = normal_values(streams_of[11], (REQS, D), 1.0, 6.0, ((0, 128),))
    norm_gain = jnp.clip(1.0 + 0.18 * jax.random.normal(streams_of[12], (D,), jnp.float32), 0.1, 1.9)
    expert_ids_keys = jax.random.split(jax.random.fold_in(streams_of[13], 1), REQS // TOK_DEV)
    expert_ids_turns = jax.random.permutation(jax.random.fold_in(streams_of[13], 3), REQS // TOK_DEV)
    expert_ids = jax.vmap(lambda own, number: shared_out(jax.random.fold_in(streams_of[13], 2), own, number, TOK_DEV, EXPERTS, TOP, CAPE, 2))(expert_ids_keys, expert_ids_turns).reshape((REQS, TOP))
    gate_weights = jnp.clip(0.1 + 0.79999997 * jax.random.uniform(streams_of[14], (REQS, TOP), jnp.float32) ** level_of(streams_of[14], (REQS, TOP), ((0, 128),), -0.2, 0.2), 0.1, 0.9)
    w_gate = normal_values(streams_of[15], (EXPERTS, D, FF), D ** -0.5, 0.09375, ((0, 8), (2, 16)))
    w_up = normal_values(streams_of[16], (EXPERTS, D, FF), D ** -0.5, 0.09375, ((0, 8), (2, 16)))
    w_down = normal_values(streams_of[17], (EXPERTS, FF, D), FF ** -0.5, 0.046875, ((0, 8), (1, 16)))
    return dict(query=query, new_key=new_key, new_value=new_value, private_keys=private_keys, private_values=private_values, private_lengths=private_lengths, prefix_keys=prefix_keys, prefix_values=prefix_values, slot_group=slot_group, group_ids=group_ids, out_weight=out_weight, hidden_in=hidden_in, norm_gain=norm_gain, expert_ids=expert_ids, gate_weights=gate_weights, w_gate=w_gate, w_up=w_up, w_down=w_down)


NEG = -1e+30
EPSILON = 1e-05

def reference(query, new_key, new_value, private_keys, private_values, private_lengths, prefix_keys, prefix_values, slot_group, group_ids, out_weight, hidden_in, norm_gain, expert_ids, gate_weights, w_gate, w_up, w_down):
    floats = jnp.float32
    scale = 1.0 / math.sqrt(HEAD_DIM)
    queries = query.astype(floats).reshape(REQS, KV_HEADS, QPK, HEAD_DIM)
    own_keys = private_keys.astype(floats).reshape(REQS, PRIV, KV_HEADS, HEAD_DIM)
    own_values = private_values.astype(floats).reshape(REQS, PRIV, KV_HEADS, HEAD_DIM)
    scores = jnp.einsum('rkqd,rpkd->rkqp', queries, own_keys) * scale
    live = jnp.arange(PRIV, dtype=jnp.int32)[None, :] < private_lengths[:, None]
    live4 = live[:, None, None, :]
    scores = jnp.where(live4, scores, NEG)
    fresh = jnp.einsum('rkqd,rkd->rkq', queries, new_key.astype(floats).reshape(REQS, KV_HEADS, HEAD_DIM)) * scale
    top = jnp.maximum(lax.optimization_barrier(jnp.max(scores, axis=-1)), fresh)
    expo = jnp.where(live4, jnp.exp(scores - top[..., None]), 0.0)
    fresh_expo = jnp.exp(fresh - top)
    total = lax.optimization_barrier(jnp.sum(expo, axis=-1)) + fresh_expo
    weights = lax.optimization_barrier(expo.astype(jnp.bfloat16)).astype(floats)
    fresh_weights = lax.optimization_barrier(fresh_expo.astype(jnp.bfloat16)).astype(floats)
    summed = jnp.einsum('rkqp,rpkd->rkqd', weights, own_values)
    summed = summed + fresh_weights[..., None] * new_value.astype(floats).reshape(REQS, KV_HEADS, 1, HEAD_DIM)
    near_out = summed / total[..., None]
    near_lse = top + jnp.log(total)
    matches = group_ids[:, 0][:, None] == slot_group[None, :]
    slot = lax.optimization_barrier(jnp.sum(jnp.where(matches, jnp.arange(GROUPS, dtype=jnp.int32)[None, :], 0), axis=1)).astype(jnp.int32)
    blocks = REQS // R_DEV

    def prefix_block(items):
        block_queries, block_slots = items
        keys = prefix_keys[block_slots].astype(floats).reshape(-1, PLEN, KV_HEADS, HEAD_DIM)
        values = prefix_values[block_slots].astype(floats).reshape(-1, PLEN, KV_HEADS, HEAD_DIM)
        block_scores = jnp.einsum('rkqd,rpkd->rkqp', block_queries, keys) * scale
        block_top = lax.optimization_barrier(jnp.max(block_scores, axis=-1))
        block_expo = jnp.exp(block_scores - block_top[..., None])
        block_total = lax.optimization_barrier(jnp.sum(block_expo, axis=-1))
        block_weights = lax.optimization_barrier(block_expo.astype(jnp.bfloat16)).astype(floats)
        block_sum = jnp.einsum('rkqp,rpkd->rkqd', block_weights, values)
        return (block_sum / block_total[..., None], block_top + jnp.log(block_total))
    far_out, far_lse = lax.map(prefix_block, (queries.reshape(blocks, R_DEV, KV_HEADS, QPK, HEAD_DIM), slot.reshape(blocks, R_DEV)))
    far_out = far_out.reshape(REQS, KV_HEADS, QPK, HEAD_DIM)
    far_lse = far_lse.reshape(REQS, KV_HEADS, QPK)
    both = jnp.logaddexp(near_lse, far_lse)
    merged = near_out * jnp.exp(near_lse - both)[..., None] + far_out * jnp.exp(far_lse - both)[..., None]
    attention = merged.reshape(REQS, QW).astype(jnp.bfloat16)
    proj = jnp.dot(attention, out_weight, preferred_element_type=jnp.float32)
    resid = hidden_in.astype(floats) + proj
    normed = (resid * lax.rsqrt(lax.optimization_barrier(jnp.mean(resid * resid, axis=-1, keepdims=True)) + EPSILON) * norm_gain).astype(jnp.bfloat16)
    capacity = N_CACHE * N_EXPERT * CAPE

    def one_expert(index):
        hit = expert_ids == index
        chosen = jnp.any(hit, axis=1)
        weight = lax.optimization_barrier(jnp.sum(jnp.where(hit, gate_weights, 0.0), axis=1))
        place = (jnp.cumsum(chosen.astype(jnp.int32)) - 1).astype(jnp.int32)
        target = jnp.where(chosen, place, capacity).astype(jnp.int32)
        rows = jnp.zeros((capacity,), jnp.int32).at[target].set(jnp.arange(REQS, dtype=jnp.int32), mode='drop')
        picked = normed[rows]
        gate = jnp.dot(picked, w_gate[index], preferred_element_type=jnp.float32)
        up = jnp.dot(picked, w_up[index], preferred_element_type=jnp.float32)
        act = (jax.nn.silu(gate) * up).astype(jnp.bfloat16)
        out = jnp.dot(act, w_down[index], preferred_element_type=jnp.float32).astype(jnp.bfloat16)
        back = out[jnp.clip(place, 0, capacity - 1)].astype(floats)
        return weight[:, None] * back
    moe = lax.optimization_barrier(jnp.sum(lax.map(one_expert, jnp.arange(EXPERTS, dtype=jnp.int32)), axis=0))
    layer_out = (resid + moe).astype(jnp.bfloat16)
    return (attention, layer_out)
```

```python
import math

import jax
import jax.numpy as jnp
from jax import lax
from jax.sharding import Mesh
from jax.sharding import PartitionSpec as P

MOSTG = 8
CACHE = ("x", "z")
CACHE_EXPERT = ("x", "z", "y", "k")
RING = 4
GROUPS_OF_CHUNKS = ((0,), (1,), (3,), (2,))

NEG = -1e30
EPSILON = 1e-05
F32 = jnp.float32
BF16 = jnp.bfloat16


def push(block, axis, distance):
    if distance == 0:
        return block
    return lax.ppermute(block, axis, [(i, (i + distance) % RING) for i in range(RING)])


def swap(block):
    return lax.ppermute(block, "k", [(0, 1), (1, 0)])


def private_partial(queries, keys, values, lengths, new_key, new_value, scale):
    scores = jnp.einsum("rhd,rpd->rhp", queries, keys, preferred_element_type=F32) * scale
    live = jnp.arange(keys.shape[1], dtype=jnp.int32)[None, :] < lengths[:, None]
    scores = jnp.where(live[:, None, :], scores, NEG)
    fresh = jnp.einsum("rhd,rd->rh", queries, new_key, preferred_element_type=F32) * scale
    top = jnp.maximum(jnp.max(scores, axis=-1), fresh)
    expo = jnp.where(live[:, None, :], jnp.exp(scores - top[..., None]), 0.0)
    fresh_expo = jnp.exp(fresh - top)
    total = jnp.sum(expo, axis=-1) + fresh_expo
    summed = jnp.einsum("rhp,rpd->rhd", expo.astype(BF16), values, preferred_element_type=F32)
    summed = summed + fresh_expo[..., None] * new_value.astype(F32)[:, None, :]
    return (summed / total[..., None], top + jnp.log(total))


def prefix_partial(received, prefix_keys, prefix_values, scale):
    rows, heads, width = received.shape
    slots = prefix_keys.shape[0]
    blocks = received.reshape(rows // (slots * MOSTG), slots, MOSTG, heads, width)
    scores = jnp.einsum("cgmhd,gpd->cgmhp", blocks, prefix_keys, preferred_element_type=F32) * scale
    top = jnp.max(scores, axis=-1)
    expo = jnp.exp(scores - top[..., None])
    total = jnp.sum(expo, axis=-1)
    summed = jnp.einsum(
        "cgmhp,gpd->cgmhd", expo.astype(BF16), prefix_values, preferred_element_type=F32
    )
    outputs = (summed / total[..., None]).reshape(rows, heads * width)
    return (outputs, (top + jnp.log(total)).reshape(rows, heads))


def in_pieces(value):
    first = lax.reduce_precision(value, 8, 7)
    rest = value - first
    second = lax.reduce_precision(rest, 8, 7)
    return (first, second, rest - second)


def on_device(
    query,
    new_key,
    new_value,
    private_keys,
    private_values,
    private_lengths,
    prefix_keys,
    prefix_values,
    slot_group,
    group_ids,
    out_weight,
    hidden_in,
    norm_gain,
    expert_ids,
    gate_weights,
    w_gate,
    w_up,
    w_down,
):
    at_x, at_z, at_y, at_k = (lax.axis_index(name) for name in CACHE_EXPERT)
    head_dim = new_key.shape[1]
    requests = query.shape[0]
    heads = query.shape[1] // head_dim
    width = heads * head_dim
    scale = 1.0 / math.sqrt(head_dim)
    experts = 2 * RING
    tokens = hidden_in.shape[0]

    slot_count = slot_group.shape[0]
    matches = group_ids[:, 0][:, None] == slot_group[None, :]
    slot = jnp.sum(jnp.where(matches, jnp.arange(slot_count, dtype=jnp.int32)[None, :], 0), axis=1)
    order = jnp.arange(requests, dtype=jnp.int32)
    earlier = order[None, :] < order[:, None]
    rank = jnp.sum((slot[:, None] == slot[None, :]) & earlier, axis=1)
    position = slot * MOSTG + rank
    places = jnp.arange(slot_count * MOSTG, dtype=jnp.int32)
    placing = (places[:, None] == position[None, :]).astype(BF16)
    sent = jnp.dot(placing, query, preferred_element_type=F32).astype(BF16)
    received = lax.all_to_all(sent, CACHE, split_axis=0, concat_axis=0, tiled=True)

    weights = jnp.stack([push(out_weight, "x", -j) for j in range(RING)])

    queries = query.reshape(requests, heads, head_dim)
    near_out, near_lse = private_partial(
        queries, private_keys, private_values, private_lengths, new_key, new_value, scale
    )

    outputs, lse_part = prefix_partial(
        received.reshape(slot_count * MOSTG, heads, head_dim), prefix_keys, prefix_values, scale
    )
    pieces = jnp.concatenate(in_pieces(lse_part), axis=1)
    pieces = jnp.pad(pieces, ((0, 0), (0, 128 - 3 * heads)))
    back = lax.all_to_all(
        jnp.concatenate([outputs.astype(BF16), pieces.astype(BF16)], axis=1),
        CACHE,
        split_axis=0,
        concat_axis=0,
        tiled=True,
    )
    taken = lax.dot_general(placing, back, (((0,), (0,)), ((), ())), preferred_element_type=F32)
    far_out = taken[:, :width].reshape(requests, heads, head_dim)
    far_lse = taken[:, width : width + 3 * heads].reshape(requests, 3, heads).sum(axis=1)
    both = jnp.logaddexp(near_lse, far_lse)
    merged = (
        near_out * jnp.exp(near_lse - both)[..., None]
        + far_out * jnp.exp(far_lse - both)[..., None]
    )
    attention = merged.astype(BF16).reshape(requests, width)

    rows = attention.reshape(RING, 2, tokens, width)
    rows = jnp.where(at_k == 0, rows, rows[:, ::-1])
    rows = lax.dynamic_slice_in_dim(jnp.concatenate([rows, rows]), at_y, RING, 0)
    gathered = jnp.stack([push(rows, "z", i) for i in range(RING)]).reshape(-1, width)
    terms = jnp.stack(
        [jnp.dot(gathered, weights[j], preferred_element_type=F32) for j in range(RING)], axis=1
    ).reshape(RING, RING, 2, tokens, -1)
    halved = terms[:, :, 0] + swap(terms[:, :, 1].astype(BF16)).astype(F32)
    halved = halved.astype(BF16)
    reduced = sum(push(halved[:, j], "y", j).astype(F32) for j in range(RING)).astype(BF16)
    spread = jnp.stack([push(reduced[i], "z", -i) for i in range(RING)])
    spread = spread.reshape(RING, tokens, RING, -1)
    spread = lax.dynamic_slice_in_dim(
        jnp.concatenate([spread, spread]), (RING - at_z) % RING, RING, 0
    )
    spread = lax.dynamic_slice_in_dim(
        jnp.concatenate([spread, spread], axis=2), (RING - at_x) % RING, RING, 2
    )
    proj = spread.transpose(1, 2, 0, 3).reshape(tokens, -1).astype(F32)
    resid = hidden_in.astype(F32) + proj
    normed = (
        resid * lax.rsqrt(jnp.mean(resid * resid, axis=-1, keepdims=True) + EPSILON) * norm_gain
    ).astype(BF16)

    capacity = max(2, 4 * tokens // experts)
    flat_ids = expert_ids.reshape(-1)
    order_ids = jnp.arange(flat_ids.shape[0], dtype=jnp.int32)
    before = order_ids[None, :] < order_ids[:, None]
    slot_rank = jnp.sum((flat_ids[:, None] == flat_ids[None, :]) & before, axis=1)
    away = (flat_ids // 2 - at_y) % RING
    other = (flat_ids % 2 + at_k) % 2
    destination = (away * 2 + other) * capacity + slot_rank
    expert_slots = jnp.arange(experts * capacity, dtype=jnp.int32)
    chosen = (destination[None, :] == expert_slots[:, None]).reshape(experts * capacity, tokens, 2)
    picking = jnp.sum(chosen.astype(BF16), axis=2)
    outgoing = jnp.dot(picking, normed, preferred_element_type=F32).astype(BF16)
    outgoing = outgoing.reshape(RING, 2, capacity, -1)
    own = jnp.stack([outgoing[:, 0], swap(outgoing[:, 1])], axis=1)
    arrived = jnp.stack([push(own[j], "y", j) for j in range(RING)])
    arrived = arrived.reshape(experts * capacity, -1)

    half = experts * capacity // 2
    first = jnp.stack([push(arrived[:half], "x", j) for j in range(RING)])
    second = jnp.stack([push(arrived[half:], "z", j) for j in range(RING)])

    def apply(piece):
        gate = jnp.dot(piece, w_gate[0], preferred_element_type=F32)
        up = jnp.dot(piece, w_up[0], preferred_element_type=F32)
        act = (jax.nn.silu(gate) * up).astype(BF16)
        return jnp.dot(act, w_down[0], preferred_element_type=F32).astype(BF16)

    here = {}
    for d in (0, 1, 3, 2):
        here[d] = jnp.stack([push(first, "z", d), push(second, "x", d)])
    sums = None
    for group in GROUPS_OF_CHUNKS:
        piece = jnp.stack([here[d] for d in group])
        done = apply(piece.reshape(-1, piece.shape[-1])).reshape(piece.shape)
        for place, d in enumerate(group):
            parts = [push(done[place, 0], "z", -d), push(done[place, 1], "x", -d)]
            parts = [part.astype(F32) for part in parts]
            sums = parts if sums is None else [a + b for a, b in zip(sums, parts)]
    first, second = (part.astype(BF16) for part in sums)
    first = sum(push(first[j], "x", -j).astype(F32) for j in range(RING))
    second = sum(push(second[j], "z", -j).astype(F32) for j in range(RING))
    summed = jnp.concatenate([first, second]).astype(BF16).reshape(RING, 2, capacity, -1)

    own = jnp.stack([push(summed[j], "y", -j) for j in range(RING)])
    returned = jnp.stack([own[:, 0], swap(own[:, 1])], axis=1).reshape(experts * capacity, -1)
    mixing = jnp.sum(jnp.where(chosen, gate_weights[None, :, :], 0.0), axis=2)
    moe = jnp.einsum("st,sd->td", mixing, returned.astype(F32), precision=lax.Precision.HIGHEST)
    layer_out = (resid + moe).astype(BF16)
    return (attention, layer_out)


def solution(mesh):
    split = Mesh(mesh.devices.reshape(RING, RING, RING, 2), CACHE_EXPERT)
    expert = ("y", "k")
    in_specs = (
        P(CACHE, expert),
        P(CACHE, expert),
        P(CACHE, expert),
        P(CACHE, None, expert),
        P(CACHE, None, expert),
        P(CACHE),
        P(CACHE, None, expert),
        P(CACHE, None, expert),
        P(),
        P(CACHE, None),
        P(expert, CACHE),
        P(CACHE_EXPERT, None),
        P(),
        P(CACHE_EXPERT, None),
        P(CACHE_EXPERT, None),
        P(expert, None, CACHE),
        P(expert, None, CACHE),
        P(expert, CACHE, None),
    )
    out_specs = (P(CACHE, expert), P(CACHE_EXPERT, None))
    return jax.shard_map(
        on_device, mesh=split, in_specs=in_specs, out_specs=out_specs, check_vma=False
    )
```

```python
import math

import jax
import jax.numpy as jnp
from jax import lax
from jax.experimental import pallas as pl
from jax.experimental.pallas import tpu as pltpu
from jax.sharding import Mesh
from jax.sharding import PartitionSpec as P

MOSTG = 8
CACHE = ("x", "z")
CACHE_EXPERT = ("x", "z", "y", "k")
RING = 4
VLIM = 16
N_BLOCK = 1024

NEG = -1e30
EPSILON = 1e-05
F32 = jnp.float32
BF16 = jnp.bfloat16


def push(block, axis, distance):
    if distance == 0:
        return block
    return lax.ppermute(block, axis, [(i, (i + distance) % RING) for i in range(RING)])


def turn(block, stage, distance):
    if distance == 0:
        return block
    pairs = []
    for x in range(RING):
        for z in range(RING):
            for k in range(2):
                along_x = (k + stage) % 2 == 0
                to_x = (x + distance) % RING if along_x else x
                to_z = z if along_x else (z + distance) % RING
                pairs.append(((x * RING + z) * 2 + k, (to_x * RING + to_z) * 2 + k))
    return lax.ppermute(block, ("x", "z", "k"), pairs)


def swap(block):
    return lax.ppermute(block, "k", [(0, 1), (1, 0)])


def private_partial(queries, keys, values, lengths, new_key, new_value, scale):
    scores = jnp.einsum("rhd,rpd->rhp", queries, keys, preferred_element_type=F32) * scale
    live = jnp.arange(keys.shape[1], dtype=jnp.int32)[None, :] < lengths[:, None]
    scores = jnp.where(live[:, None, :], scores, NEG)
    fresh = jnp.einsum("rhd,rd->rh", queries, new_key, preferred_element_type=F32) * scale
    top = jnp.maximum(jnp.max(scores, axis=-1), fresh)
    expo = jnp.where(live[:, None, :], jnp.exp(scores - top[..., None]), 0.0)
    fresh_expo = jnp.exp(fresh - top)
    total = jnp.sum(expo, axis=-1) + fresh_expo
    summed = jnp.einsum("rhp,rpd->rhd", expo.astype(BF16), values, preferred_element_type=F32)
    summed = summed + fresh_expo[..., None] * new_value.astype(F32)[:, None, :]
    return (summed / total[..., None], top + jnp.log(total))


def in_pieces(value):
    first = lax.reduce_precision(value, 8, 7)
    rest = value - first
    second = lax.reduce_precision(rest, 8, 7)
    return (first, second, rest - second)


def prefix_kernel(heads, width, scale, received, keys, values, out):
    rows = received[...].astype(F32).reshape(-1, heads * width).astype(BF16)
    count = rows.shape[0]
    queries = jnp.concatenate([rows[:, h * width : (h + 1) * width] for h in range(heads)], axis=0)
    scores = lax.dot_general(
        queries, keys[0], (((1,), (1,)), ((), ())), preferred_element_type=F32
    )
    scores = scores * scale
    top = jnp.max(scores, axis=-1, keepdims=True)
    expo = jnp.exp(scores - top)
    total = jnp.sum(expo, axis=-1, keepdims=True)
    summed = jnp.dot(expo.astype(BF16), values[0], preferred_element_type=F32)
    outputs = summed / total
    parts = in_pieces(top + jnp.log(total))
    lane = lax.broadcasted_iota(jnp.int32, (count, width), 1)
    packed = jnp.zeros((count, width), F32)
    for p, part in enumerate(parts):
        for h in range(heads):
            packed = jnp.where(lane == p * heads + h, part[h * count : (h + 1) * count], packed)
    for h in range(heads):
        block = outputs[h * count : (h + 1) * count].reshape(-1, 1, MOSTG, width)
        out[:, :, :, h * width : (h + 1) * width] = block.astype(BF16)
    out[:, :, :, heads * width :] = packed.reshape(-1, 1, MOSTG, width).astype(BF16)


def prefix_partial(received, keys, values, heads, scale):
    slots, length, width = keys.shape
    homes = received.shape[0] // (slots * MOSTG)
    return pl.pallas_call(
        lambda *refs: prefix_kernel(heads, width, scale, *refs),
        grid=(slots,),
        in_specs=[
            pl.BlockSpec((homes, 1, MOSTG, heads * width), lambda g: (0, g, 0, 0)),
            pl.BlockSpec((1, length, width), lambda g: (g, 0, 0)),
            pl.BlockSpec((1, length, width), lambda g: (g, 0, 0)),
        ],
        out_specs=pl.BlockSpec((homes, 1, MOSTG, (heads + 1) * width), lambda g: (0, g, 0, 0)),
        out_shape=jax.ShapeDtypeStruct((homes, slots, MOSTG, (heads + 1) * width), BF16),
        compiler_params=pltpu.CompilerParams(vmem_limit_bytes=24 * 1024 * 1024),
        name="prefix_attention",
    )(
        received.reshape(homes, slots, MOSTG, heads * width),
        pltpu.with_memory_space_constraint(keys, pltpu.HBM),
        pltpu.with_memory_space_constraint(values, pltpu.HBM),
    ).reshape(
        homes * slots * MOSTG, (heads + 1) * width
    )


def expert_kernel(count, *refs):
    pieces = refs[:count]
    w_gate, w_up, w_down = refs[count : count + 3]
    outs = refs[count + 4 :]
    rows = jnp.concatenate([piece[...] for piece in pieces], axis=0)
    gate = jnp.dot(rows, w_gate[...], preferred_element_type=F32)
    up = jnp.dot(rows, w_up[...], preferred_element_type=F32)
    act = (gate / (1.0 + jnp.exp(-gate)) * up).astype(BF16)
    size = rows.shape[0] // count
    for n in range(0, w_down.shape[1], N_BLOCK):
        out = jnp.dot(act, w_down[:, n : n + N_BLOCK], preferred_element_type=F32).astype(BF16)
        for i in range(count):
            outs[i][:, n : n + N_BLOCK] = out[i * size : (i + 1) * size]


def apply_expert(pieces, weights, token):
    count = len(pieces)
    local = pl.BlockSpec(memory_space=pltpu.VMEM)
    return pl.pallas_call(
        lambda *refs: expert_kernel(count, *refs),
        in_specs=[local] * (count + 3) + [pl.BlockSpec(memory_space=pl.ANY)],
        out_specs=[local] * count,
        out_shape=[jax.ShapeDtypeStruct(pieces[0].shape, BF16)] * count,
        compiler_params=pltpu.CompilerParams(vmem_limit_bytes=VLIM * 1024 * 1024),
        name="expert_rows",
    )(*pieces, *weights, token)


def project_kernel(count, other, *refs):
    pieces = refs[:count]
    weights = refs[count : 2 * count]
    sent = refs[2 * count]
    kept = refs[2 * count + 1 :]
    for side in range(2):
        rows = jnp.concatenate([piece[side] for piece in pieces], axis=0)
        for j in range(count):
            wide = weights[j].shape[1]
            terms = jnp.dot(rows, weights[j][...], preferred_element_type=F32)
            terms = terms.reshape(count, count, -1, wide)
            for y in range(count):
                if side == other:
                    sent[y, :, :, j * wide : (j + 1) * wide] = terms[:, y].astype(BF16)
                else:
                    kept[y][:, :, j * wide : (j + 1) * wide] = terms[:, y]


def project(pieces, weights):
    count = len(pieces)
    tokens = pieces[0].shape[1] // count
    wide = sum(w.shape[1] for w in weights)
    local = pl.BlockSpec(memory_space=pltpu.VMEM)
    return pl.pallas_call(
        lambda *refs: project_kernel(count, 1, *refs),
        in_specs=[local] * (2 * count),
        out_specs=[local] * (count + 1),
        out_shape=[jax.ShapeDtypeStruct((count, count, tokens, wide), BF16)]
        + [jax.ShapeDtypeStruct((count, tokens, wide), F32)] * count,
        compiler_params=pltpu.CompilerParams(vmem_limit_bytes=16 * 1024 * 1024),
        name="project_rows",
    )(*pieces, *weights)


def load_kernel(count, *refs):
    sources, outs, sems = refs[:count], refs[count + 1 : 2 * count + 1], refs[2 * count + 1]
    copies = [
        pltpu.make_async_copy(sources[i], outs[i], sems.at[i]) for i in range(count)
    ]
    for copy in copies:
        copy.start()
    for copy in copies:
        copy.wait()


def loaded(weights, token):
    count = len(weights)
    far = pl.BlockSpec(memory_space=pl.ANY)
    outs = pl.pallas_call(
        lambda *refs: load_kernel(count, *refs),
        in_specs=[far] * (count + 1),
        out_specs=[pl.BlockSpec(memory_space=pltpu.VMEM)] * count,
        out_shape=[jax.ShapeDtypeStruct(w.shape, w.dtype) for w in weights],
        scratch_shapes=[pltpu.SemaphoreType.DMA((count,))],
        compiler_params=pltpu.CompilerParams(vmem_limit_bytes=4 * 1024 * 1024),
        name="load_weights",
    )(*[pltpu.with_memory_space_constraint(w, pltpu.HBM) for w in weights], token)
    return [pltpu.with_memory_space_constraint(w, pltpu.VMEM) for w in outs]


def on_device(
    query,
    new_key,
    new_value,
    private_keys,
    private_values,
    private_lengths,
    prefix_keys,
    prefix_values,
    slot_group,
    group_ids,
    out_weight,
    hidden_in,
    norm_gain,
    expert_ids,
    gate_weights,
    w_gate,
    w_up,
    w_down,
):
    at_x, at_z, at_y, at_k = (lax.axis_index(name) for name in CACHE_EXPERT)
    head_dim = new_key.shape[1]
    requests = query.shape[0]
    heads = query.shape[1] // head_dim
    width = heads * head_dim
    scale = 1.0 / math.sqrt(head_dim)
    experts = 2 * RING
    tokens = hidden_in.shape[0]

    slot_count = slot_group.shape[0]
    matches = group_ids[:, 0][:, None] == slot_group[None, :]
    slot = jnp.sum(jnp.where(matches, jnp.arange(slot_count, dtype=jnp.int32)[None, :], 0), axis=1)
    order = jnp.arange(requests, dtype=jnp.int32)
    earlier = order[None, :] < order[:, None]
    rank = jnp.sum((slot[:, None] == slot[None, :]) & earlier, axis=1)
    position = slot * MOSTG + rank
    places = jnp.arange(slot_count * MOSTG, dtype=jnp.int32)
    placing = (places[:, None] == position[None, :]).astype(BF16)
    sent = jnp.dot(placing, query, preferred_element_type=F32).astype(BF16)
    received = lax.all_to_all(sent, CACHE, split_axis=0, concat_axis=0, tiled=True)

    queries = query.reshape(requests, heads, head_dim)
    near_out, near_lse = private_partial(
        queries, private_keys, private_values, private_lengths, new_key, new_value, scale
    )

    partial = prefix_partial(received, prefix_keys, prefix_values, heads, scale)
    late_weight, partial = lax.optimization_barrier((out_weight, partial))
    back = lax.all_to_all(partial, CACHE, split_axis=0, concat_axis=0, tiled=True)

    weights = [push(late_weight, "x", -j) for j in range(RING)]

    taken = lax.dot_general(placing, back, (((0,), (0,)), ((), ())), preferred_element_type=F32)
    far_out = taken[:, :width].reshape(requests, heads, head_dim)
    far_lse = taken[:, width : width + 3 * heads].reshape(requests, 3, heads).sum(axis=1)
    both = jnp.logaddexp(near_lse, far_lse)
    merged = (
        near_out * jnp.exp(near_lse - both)[..., None]
        + far_out * jnp.exp(far_lse - both)[..., None]
    )
    attention = merged.astype(BF16).reshape(requests, width)

    rows = attention.reshape(RING, 2, tokens, width).transpose(1, 0, 2, 3)
    rows = jnp.where(at_k == 0, rows, rows[::-1])
    rows = lax.dynamic_slice_in_dim(jnp.concatenate([rows, rows], axis=1), at_y, RING, 1)
    rows = rows.reshape(2, RING * tokens, width)
    sent, *kept = project([push(rows, "z", i) for i in range(RING)], weights)
    sent = swap(sent)
    halved = [(kept[j] + sent[j].astype(F32)).astype(BF16) for j in range(RING)]
    reduced = sum(push(halved[j], "y", j).astype(F32) for j in range(RING)).astype(BF16)
    spread = jnp.stack([push(reduced[i], "z", -i) for i in range(RING)])
    spread = spread.reshape(RING, tokens, RING, -1)
    spread = lax.dynamic_slice_in_dim(
        jnp.concatenate([spread, spread]), (RING - at_z) % RING, RING, 0
    )
    spread = lax.dynamic_slice_in_dim(
        jnp.concatenate([spread, spread], axis=2), (RING - at_x) % RING, RING, 2
    )
    proj = spread.transpose(1, 2, 0, 3).reshape(tokens, -1).astype(F32)
    resid = hidden_in.astype(F32) + proj
    normed = (
        resid * lax.rsqrt(jnp.mean(resid * resid, axis=-1, keepdims=True) + EPSILON) * norm_gain
    ).astype(BF16)

    capacity = max(2, 4 * tokens // experts)
    flat_ids = expert_ids.reshape(-1)
    order_ids = jnp.arange(flat_ids.shape[0], dtype=jnp.int32)
    before = order_ids[None, :] < order_ids[:, None]
    slot_rank = jnp.sum((flat_ids[:, None] == flat_ids[None, :]) & before, axis=1)
    away = (flat_ids // 2 - at_y) % RING
    other = (flat_ids % 2 + at_k) % 2
    destination = (away * 2 + other) * capacity + slot_rank
    expert_slots = jnp.arange(experts * capacity, dtype=jnp.int32)
    chosen = (destination[None, :] == expert_slots[:, None]).reshape(experts * capacity, tokens, 2)
    picking = jnp.sum(chosen.astype(BF16), axis=2)
    outgoing = jnp.dot(picking, normed, preferred_element_type=F32).astype(BF16)
    outgoing = outgoing.reshape(RING, 2, capacity, -1)
    own = jnp.stack([outgoing[:, 0], swap(outgoing[:, 1])], axis=1)
    arrived = jnp.stack([push(own[j], "y", j) for j in range(RING)])
    arrived = arrived.reshape(experts * capacity, -1)

    stacked = jnp.stack([turn(arrived, 0, j) for j in range(RING)])
    near = loaded([w_gate[0], w_up[0], w_down[0]], stacked)
    rows = stacked.reshape(-1, stacked.shape[-1])
    half = rows.shape[0] // 2
    low = turn(rows, 1, 1)
    high = turn(rows, 1, -1)
    (here_out,) = apply_expert([rows], near, norm_gain)
    low, high, here_out = lax.optimization_barrier((low, high, here_out))
    across = [turn(low[:half], 1, 1), turn(high[half:], 1, -1)]
    (low_out,) = apply_expert([low], near, here_out)
    (high_out,) = apply_expert([high], near, low_out)
    across_out = apply_expert(across, near, high_out)
    from_high = turn(across_out[0], 1, -1)
    from_low = turn(across_out[1], 1, 1)
    low_out = jnp.concatenate([low_out[:half] + from_high, low_out[half:]])
    high_out = jnp.concatenate([high_out[:half], high_out[half:] + from_low])
    summed = (
        here_out.astype(F32)
        + turn(low_out, 1, -1).astype(F32)
        + turn(high_out, 1, 1).astype(F32)
    )
    summed = summed.astype(BF16).reshape(stacked.shape)
    summed = sum(turn(summed[j], 0, -j).astype(F32) for j in range(RING)).astype(BF16)
    summed = summed.reshape(RING, 2, capacity, -1)

    own = jnp.stack([push(summed[j], "y", -j) for j in range(RING)])
    returned = jnp.stack([own[:, 0], swap(own[:, 1])], axis=1).reshape(experts * capacity, -1)
    mixing = jnp.sum(jnp.where(chosen, gate_weights[None, :, :], 0.0), axis=2)
    moe = jnp.einsum("st,sd->td", mixing, returned.astype(F32), precision=lax.Precision.HIGHEST)
    layer_out = (resid + moe).astype(BF16)
    return (attention, layer_out)


def solution(mesh):
    split = Mesh(mesh.devices.reshape(RING, RING, RING, 2), CACHE_EXPERT)
    expert = ("y", "k")
    in_specs = (
        P(CACHE, expert),
        P(CACHE, expert),
        P(CACHE, expert),
        P(CACHE, None, expert),
        P(CACHE, None, expert),
        P(CACHE),
        P(CACHE, None, expert),
        P(CACHE, None, expert),
        P(),
        P(CACHE, None),
        P(expert, CACHE),
        P(CACHE_EXPERT, None),
        P(),
        P(CACHE_EXPERT, None),
        P(CACHE_EXPERT, None),
        P(expert, None, CACHE),
        P(expert, None, CACHE),
        P(expert, CACHE, None),
    )
    out_specs = (P(CACHE, expert), P(CACHE_EXPERT, None))
    return jax.shard_map(
        on_device, mesh=split, in_specs=in_specs, out_specs=out_specs, check_vma=False
    )
```

```python
import math

import jax
import jax.numpy as jnp
from jax import lax
from jax.experimental import pallas as pl
from jax.experimental.pallas import tpu as pltpu
from jax.sharding import Mesh
from jax.sharding import PartitionSpec as P

MOSTG = 8
CACHE = ("x", "z")
CACHE_EXPERT = ("x", "z", "y", "k")
RING = 4
VLIM = 16
N_BLOCK = 1024

NEG = -1e30
EPSILON = 1e-05
F32 = jnp.float32
BF16 = jnp.bfloat16


def push(block, axis, distance):
    if distance == 0:
        return block
    return lax.ppermute(block, axis, [(i, (i + distance) % RING) for i in range(RING)])


def turn(block, stage, distance):
    if distance == 0:
        return block
    pairs = []
    for x in range(RING):
        for z in range(RING):
            for k in range(2):
                along_x = (k + stage) % 2 == 0
                to_x = (x + distance) % RING if along_x else x
                to_z = z if along_x else (z + distance) % RING
                pairs.append(((x * RING + z) * 2 + k, (to_x * RING + to_z) * 2 + k))
    return lax.ppermute(block, ("x", "z", "k"), pairs)


def swap(block):
    return lax.ppermute(block, "k", [(0, 1), (1, 0)])


def private_partial(queries, keys, values, lengths, new_key, new_value, scale):
    scores = jnp.einsum("rhd,rpd->rhp", queries, keys, preferred_element_type=F32) * scale
    live = jnp.arange(keys.shape[1], dtype=jnp.int32)[None, :] < lengths[:, None]
    scores = jnp.where(live[:, None, :], scores, NEG)
    fresh = jnp.einsum("rhd,rd->rh", queries, new_key, preferred_element_type=F32) * scale
    top = jnp.maximum(jnp.max(scores, axis=-1), fresh)
    expo = jnp.where(live[:, None, :], jnp.exp(scores - top[..., None]), 0.0)
    fresh_expo = jnp.exp(fresh - top)
    total = jnp.sum(expo, axis=-1) + fresh_expo
    summed = jnp.einsum("rhp,rpd->rhd", expo.astype(BF16), values, preferred_element_type=F32)
    summed = summed + fresh_expo[..., None] * new_value.astype(F32)[:, None, :]
    return (summed / total[..., None], top + jnp.log(total))


def in_pieces(value):
    first = lax.reduce_precision(value, 8, 7)
    rest = value - first
    second = lax.reduce_precision(rest, 8, 7)
    return (first, second, rest - second)


def dispatch_kernel(group_ids, slot_group, query, sent, placing, groups, held, queries, sems):
    copies = [
        pltpu.make_async_copy(group_ids, groups, sems.at[0]),
        pltpu.make_async_copy(slot_group, held, sems.at[1]),
        pltpu.make_async_copy(query, queries, sems.at[2]),
    ]
    for copy in copies:
        copy.start()
    count, slots = groups.shape[1], held.shape[1]
    column = lax.broadcasted_iota(jnp.int32, (slots, slots), 1)
    same = lax.broadcasted_iota(jnp.int32, (slots, slots), 0) == column
    earlier = lax.broadcasted_iota(jnp.int32, (count, count), 0)
    earlier = (earlier < lax.broadcasted_iota(jnp.int32, (count, count), 1)).astype(F32)
    number = lax.broadcasted_iota(jnp.int32, (slots, count), 0).astype(F32) * MOSTG
    places = lax.broadcasted_iota(jnp.int32, (slots * MOSTG, count), 0).astype(F32)
    copies[0].wait()
    copies[1].wait()
    upright = jnp.sum(jnp.where(same, held[...].astype(F32), 0.0), axis=1, keepdims=True)
    match = (upright == groups[...].astype(F32)).astype(F32)
    before = jnp.dot(match, earlier, preferred_element_type=F32)
    position = jnp.sum(match * (number + before), axis=0, keepdims=True)
    chosen = jnp.where(places == position, 1.0, 0.0).astype(BF16)
    placing[...] = chosen
    copies[2].wait()
    sent[...] = jnp.dot(chosen, queries[...], preferred_element_type=F32).astype(BF16)


def dispatched(group_ids, slot_group, query):
    far = pl.BlockSpec(memory_space=pl.ANY)
    local = pl.BlockSpec(memory_space=pltpu.VMEM)
    count, slots = group_ids.shape[0], slot_group.shape[0]
    return pl.pallas_call(
        dispatch_kernel,
        in_specs=[far] * 3,
        out_specs=[local] * 2,
        out_shape=[
            jax.ShapeDtypeStruct((slots * MOSTG, query.shape[1]), BF16),
            jax.ShapeDtypeStruct((slots * MOSTG, count), BF16),
        ],
        scratch_shapes=[
            pltpu.VMEM((1, count), jnp.int32),
            pltpu.VMEM((1, slots), jnp.int32),
            pltpu.VMEM(query.shape, BF16),
            pltpu.SemaphoreType.DMA((3,)),
        ],
        compiler_params=pltpu.CompilerParams(vmem_limit_bytes=16 * 1024 * 1024),
        name="place_queries",
    )(
        *[
            pltpu.with_memory_space_constraint(array, pltpu.HBM)
            for array in (group_ids.reshape(1, count), slot_group.reshape(1, slots), query)
        ]
    )


def prefix_kernel(heads, width, scale, received, keys, values, out):
    rows = received[...].astype(F32).reshape(-1, heads * width).astype(BF16)
    count = rows.shape[0]
    lane = lax.broadcasted_iota(jnp.int32, (count, width), 1)
    packed = jnp.zeros((count, width), F32)
    for h in range(heads):
        scores = lax.dot_general(
            rows[:, h * width : (h + 1) * width],
            keys[0],
            (((1,), (1,)), ((), ())),
            preferred_element_type=F32,
        )
        top = jnp.max(scores, axis=-1, keepdims=True)
        expo = jnp.exp2((scores - top) * (scale * math.log2(math.e)))
        total = jnp.sum(expo, axis=-1, keepdims=True)
        summed = jnp.dot(expo.astype(BF16), values[0], preferred_element_type=F32)
        block = (summed / total).reshape(-1, 1, MOSTG, width)
        out[:, :, :, h * width : (h + 1) * width] = block.astype(BF16)
        for p, part in enumerate(in_pieces(top * scale + jnp.log(total))):
            packed = jnp.where(lane == p * heads + h, part, packed)
    out[:, :, :, heads * width :] = packed.reshape(-1, 1, MOSTG, width).astype(BF16)


def prefix_partial(received, keys, values, heads, scale):
    slots, length, width = keys.shape
    homes = received.shape[0] // (slots * MOSTG)
    return pl.pallas_call(
        lambda *refs: prefix_kernel(heads, width, scale, *refs),
        grid=(slots,),
        in_specs=[
            pl.BlockSpec((homes, 1, MOSTG, heads * width), lambda g: (0, g, 0, 0)),
            pl.BlockSpec((1, length, width), lambda g: (g, 0, 0)),
            pl.BlockSpec((1, length, width), lambda g: (g, 0, 0)),
        ],
        out_specs=pl.BlockSpec((homes, 1, MOSTG, (heads + 1) * width), lambda g: (0, g, 0, 0)),
        out_shape=jax.ShapeDtypeStruct((homes, slots, MOSTG, (heads + 1) * width), BF16),
        compiler_params=pltpu.CompilerParams(vmem_limit_bytes=24 * 1024 * 1024),
        name="prefix_attention",
    )(
        received.reshape(homes, slots, MOSTG, heads * width),
        pltpu.with_memory_space_constraint(keys, pltpu.HBM),
        pltpu.with_memory_space_constraint(values, pltpu.HBM),
    ).reshape(
        homes * slots * MOSTG, (heads + 1) * width
    )


def expert_kernel(count, *refs):
    pieces = refs[:count]
    w_gate, w_up, w_down = refs[count : count + 3]
    outs = refs[count + 4 :]
    rows = jnp.concatenate([piece[...] for piece in pieces], axis=0)
    gate = jnp.dot(rows, w_gate[...], preferred_element_type=F32)
    up = jnp.dot(rows, w_up[...], preferred_element_type=F32)
    act = (gate / (1.0 + jnp.exp(-gate)) * up).astype(BF16)
    size = rows.shape[0] // count
    for n in range(0, w_down.shape[1], N_BLOCK):
        out = jnp.dot(act, w_down[:, n : n + N_BLOCK], preferred_element_type=F32).astype(BF16)
        for i in range(count):
            outs[i][:, n : n + N_BLOCK] = out[i * size : (i + 1) * size]


def apply_expert(pieces, weights, token):
    count = len(pieces)
    local = pl.BlockSpec(memory_space=pltpu.VMEM)
    return pl.pallas_call(
        lambda *refs: expert_kernel(count, *refs),
        in_specs=[local] * (count + 3) + [pl.BlockSpec(memory_space=pl.ANY)],
        out_specs=[local] * count,
        out_shape=[jax.ShapeDtypeStruct(pieces[0].shape, BF16)] * count,
        compiler_params=pltpu.CompilerParams(vmem_limit_bytes=VLIM * 1024 * 1024),
        name="expert_rows",
    )(*pieces, *weights, token)


def project_kernel(count, other, *refs):
    pieces = refs[:count]
    weights = refs[count : 2 * count]
    sent = refs[2 * count]
    kept = refs[2 * count + 1 :]
    for side in range(2):
        rows = jnp.concatenate([piece[side] for piece in pieces], axis=0)
        for j in range(count):
            wide = weights[j].shape[1]
            terms = jnp.dot(rows, weights[j][...], preferred_element_type=F32)
            terms = terms.reshape(count, count, -1, wide)
            for y in range(count):
                if side == other:
                    sent[y, :, :, j * wide : (j + 1) * wide] = terms[:, y].astype(BF16)
                else:
                    kept[y][:, :, j * wide : (j + 1) * wide] = terms[:, y]


def project(pieces, weights):
    count = len(pieces)
    tokens = pieces[0].shape[1] // count
    wide = sum(w.shape[1] for w in weights)
    local = pl.BlockSpec(memory_space=pltpu.VMEM)
    return pl.pallas_call(
        lambda *refs: project_kernel(count, 1, *refs),
        in_specs=[local] * (2 * count),
        out_specs=[local] * (count + 1),
        out_shape=[jax.ShapeDtypeStruct((count, count, tokens, wide), BF16)]
        + [jax.ShapeDtypeStruct((count, tokens, wide), F32)] * count,
        compiler_params=pltpu.CompilerParams(vmem_limit_bytes=16 * 1024 * 1024),
        name="project_rows",
    )(*pieces, *weights)


def load_kernel(count, *refs):
    sources, outs, sems = refs[:count], refs[count + 1 : 2 * count + 1], refs[2 * count + 1]
    copies = [
        pltpu.make_async_copy(sources[i], outs[i], sems.at[i]) for i in range(count)
    ]
    for copy in copies:
        copy.start()
    for copy in copies:
        copy.wait()


def loaded(weights, token):
    count = len(weights)
    far = pl.BlockSpec(memory_space=pl.ANY)
    outs = pl.pallas_call(
        lambda *refs: load_kernel(count, *refs),
        in_specs=[far] * (count + 1),
        out_specs=[pl.BlockSpec(memory_space=pltpu.VMEM)] * count,
        out_shape=[jax.ShapeDtypeStruct(w.shape, w.dtype) for w in weights],
        scratch_shapes=[pltpu.SemaphoreType.DMA((count,))],
        compiler_params=pltpu.CompilerParams(vmem_limit_bytes=4 * 1024 * 1024),
        name="load_weights",
    )(*[pltpu.with_memory_space_constraint(w, pltpu.HBM) for w in weights], token)
    return [pltpu.with_memory_space_constraint(w, pltpu.VMEM) for w in outs]


def on_device(
    query,
    new_key,
    new_value,
    private_keys,
    private_values,
    private_lengths,
    prefix_keys,
    prefix_values,
    slot_group,
    group_ids,
    out_weight,
    hidden_in,
    norm_gain,
    expert_ids,
    gate_weights,
    w_gate,
    w_up,
    w_down,
):
    at_x, at_z, at_y, at_k = (lax.axis_index(name) for name in CACHE_EXPERT)
    head_dim = new_key.shape[1]
    requests = query.shape[0]
    heads = query.shape[1] // head_dim
    width = heads * head_dim
    scale = 1.0 / math.sqrt(head_dim)
    experts = 2 * RING
    tokens = hidden_in.shape[0]

    sent, placing = dispatched(group_ids, slot_group, query)
    received = lax.all_to_all(sent, CACHE, split_axis=0, concat_axis=0, tiled=True)

    queries = query.reshape(requests, heads, head_dim)
    near_out, near_lse = private_partial(
        queries, private_keys, private_values, private_lengths, new_key, new_value, scale
    )

    partial = prefix_partial(received, prefix_keys, prefix_values, heads, scale)
    late_weight, partial = lax.optimization_barrier((out_weight, partial))
    back = lax.all_to_all(partial, CACHE, split_axis=0, concat_axis=0, tiled=True)

    weights = [push(late_weight, "x", -j) for j in range(RING)]

    taken = lax.dot_general(placing, back, (((0,), (0,)), ((), ())), preferred_element_type=F32)
    far_out = taken[:, :width].reshape(requests, heads, head_dim)
    far_lse = taken[:, width : width + 3 * heads].reshape(requests, 3, heads).sum(axis=1)
    both = jnp.logaddexp(near_lse, far_lse)
    merged = (
        near_out * jnp.exp(near_lse - both)[..., None]
        + far_out * jnp.exp(far_lse - both)[..., None]
    )
    attention = merged.astype(BF16).reshape(requests, width)

    rows = attention.reshape(RING, 2, tokens, width).transpose(1, 0, 2, 3)
    rows = jnp.where(at_k == 0, rows, rows[::-1])
    rows = lax.dynamic_slice_in_dim(jnp.concatenate([rows, rows], axis=1), at_y, RING, 1)
    rows = rows.reshape(2, RING * tokens, width)
    sent, *kept = project([push(rows, "z", i) for i in range(RING)], weights)
    sent = swap(sent)
    halved = [(kept[j] + sent[j].astype(F32)).astype(BF16) for j in range(RING)]
    reduced = sum(push(halved[j], "y", j).astype(F32) for j in range(RING)).astype(BF16)
    spread = jnp.stack([push(reduced[i], "z", -i) for i in range(RING)])
    spread = spread.reshape(RING, tokens, RING, -1)
    spread = lax.dynamic_slice_in_dim(
        jnp.concatenate([spread, spread]), (RING - at_z) % RING, RING, 0
    )
    spread = lax.dynamic_slice_in_dim(
        jnp.concatenate([spread, spread], axis=2), (RING - at_x) % RING, RING, 2
    )
    proj = spread.transpose(1, 2, 0, 3).reshape(tokens, -1).astype(F32)
    resid = hidden_in.astype(F32) + proj
    normed = (
        resid * lax.rsqrt(jnp.mean(resid * resid, axis=-1, keepdims=True) + EPSILON) * norm_gain
    ).astype(BF16)

    capacity = max(2, 4 * tokens // experts)
    flat_ids = expert_ids.reshape(-1)
    order_ids = jnp.arange(flat_ids.shape[0], dtype=jnp.int32)
    before = order_ids[None, :] < order_ids[:, None]
    slot_rank = jnp.sum((flat_ids[:, None] == flat_ids[None, :]) & before, axis=1)
    away = (flat_ids // 2 - at_y) % RING
    other = (flat_ids % 2 + at_k) % 2
    destination = (away * 2 + other) * capacity + slot_rank
    expert_slots = jnp.arange(experts * capacity, dtype=jnp.int32)
    chosen = (destination[None, :] == expert_slots[:, None]).reshape(experts * capacity, tokens, 2)
    picking = jnp.sum(chosen.astype(BF16), axis=2)
    outgoing = jnp.dot(picking, normed, preferred_element_type=F32).astype(BF16)
    outgoing = outgoing.reshape(RING, 2, capacity, -1)
    own = jnp.stack([outgoing[:, 0], swap(outgoing[:, 1])], axis=1)
    arrived = jnp.stack([push(own[j], "y", j) for j in range(RING)])
    arrived = arrived.reshape(experts * capacity, -1)

    stacked = jnp.stack([turn(arrived, 0, j) for j in range(RING)])
    near = loaded([w_gate[0], w_up[0], w_down[0]], stacked)
    rows = stacked.reshape(-1, stacked.shape[-1])
    half = rows.shape[0] // 2
    low = turn(rows, 1, 1)
    high = turn(rows, 1, -1)
    (here_out,) = apply_expert([rows], near, norm_gain)
    low, high, here_out = lax.optimization_barrier((low, high, here_out))
    across = [turn(low[:half], 1, 1), turn(high[half:], 1, -1)]
    (low_out,) = apply_expert([low], near, here_out)
    (high_out,) = apply_expert([high], near, low_out)
    across_out = apply_expert(across, near, high_out)
    from_high = turn(across_out[0], 1, -1)
    from_low = turn(across_out[1], 1, 1)
    low_out = jnp.concatenate([low_out[:half] + from_high, low_out[half:]])
    high_out = jnp.concatenate([high_out[:half], high_out[half:] + from_low])
    summed = (
        here_out.astype(F32)
        + turn(low_out, 1, -1).astype(F32)
        + turn(high_out, 1, 1).astype(F32)
    )
    summed = summed.astype(BF16).reshape(stacked.shape)
    summed = sum(turn(summed[j], 0, -j).astype(F32) for j in range(RING)).astype(BF16)
    summed = summed.reshape(RING, 2, capacity, -1)

    own = jnp.stack([push(summed[j], "y", -j) for j in range(RING)])
    returned = jnp.stack([own[:, 0], swap(own[:, 1])], axis=1).reshape(experts * capacity, -1)
    mixing = jnp.sum(jnp.where(chosen, gate_weights[None, :, :], 0.0), axis=2)
    moe = jnp.einsum("st,sd->td", mixing, returned.astype(F32), precision=lax.Precision.HIGHEST)
    layer_out = (resid + moe).astype(BF16)
    return (attention, layer_out)


def solution(mesh):
    split = Mesh(mesh.devices.reshape(RING, RING, RING, 2), CACHE_EXPERT)
    expert = ("y", "k")
    in_specs = (
        P(CACHE, expert),
        P(CACHE, expert),
        P(CACHE, expert),
        P(CACHE, None, expert),
        P(CACHE, None, expert),
        P(CACHE),
        P(CACHE, None, expert),
        P(CACHE, None, expert),
        P(),
        P(CACHE, None),
        P(expert, CACHE),
        P(CACHE_EXPERT, None),
        P(),
        P(CACHE_EXPERT, None),
        P(CACHE_EXPERT, None),
        P(expert, None, CACHE),
        P(expert, None, CACHE),
        P(expert, CACHE, None),
    )
    out_specs = (P(CACHE, expert), P(CACHE_EXPERT, None))
    return jax.shard_map(
        on_device, mesh=split, in_specs=in_specs, out_specs=out_specs, check_vma=False
    )
```
